32 devices in a mesh: batch: 16 (over z, x, core), seq: 2 (over y).
Axes of the slice: x: 2, y: 2, z: 4, core: 2. Of those that a mesh axis runs over, the one named last changes fastest.
Arguments:
- tokens: bfloat16 [16, 1024, 2560], P('batch', 'seq'), may hold values from -6 to 6
- attn_in: bfloat16 [16, 1024, 2560], P('batch', 'seq'), may hold values from -6 to 6
- lengths: int32 [16], P('batch'), may hold values from 256 to 1024
- norm_gain: float32 [2560], replicated, may hold values from 0.5 to 1.5
- attn_gain: float32 [2560], replicated, may hold values from 0.5 to 1.5
- w_x: bfloat16 [2560, 2560], P(('batch', 'seq')), may hold values from -0.125 to 0.125
- conv_w: float32 [4, 2560], replicated, may hold values from -3 to 3
- w_a: bfloat16 [10, 256, 256], replicated, may hold values from -0.375 to 0.375
- w_i: bfloat16 [10, 256, 256], replicated, may hold values from -0.375 to 0.375
- lru_decay: float32 [2560], replicated, may hold values from 4 to 20
- w_kv: bfloat16 [2560, 512], replicated, may hold values from -0.125 to 0.125
Outputs:
- lru_state: float32 [16, 2560], P('batch', 'seq')
- conv_state: bfloat16 [16, 3, 2560], P('batch', None, 'seq')
- kv_cache: bfloat16 [16, 2048, 512], P('batch', None, 'seq')
The draws below stay inside these ranges and needn't reach their ends.
Inputs may be any that keep to these rules, and one draw needn't show every extreme that they name: `lengths`: positions from a prompt's length on are padding.
All inputs are finite; a program needn't handle non-finite values.
Results may differ from the reference program's by a relative error of at most 0.0051.
Values may be sent and summed in bfloat16 or wider, within the bound.
A program may use at most 128 MiB of HBM per device.

```python
import jax
import jax.numpy as jnp
from jax import lax

D = 2560
H = 10
HD = 256
W = 2048
SEQ = 1024
PROMPTS = 16


def draw_lru_decay(key, part):
    pick_key = jax.random.fold_in(key, 11)
    slow_key = jax.random.fold_in(key, 12)
    fast_key = jax.random.fold_in(key, 13)
    share = 50
    fast_mask = jax.random.randint(pick_key, (D,), 0, 100) < share
    slow_value = jnp.log(8.0 * SEQ / jax.random.uniform(slow_key, (D,), jnp.float32, 0.2, 1.0))
    fast_value = jnp.log(jax.random.uniform(fast_key, (D,), jnp.float32, 120.0, 200.0))
    return jnp.where(fast_mask, fast_value, slow_value).astype(jnp.float32)


def place_ends(array, own_key, smallest, largest):
    index_at = [jax.random.randint(jax.random.fold_in(own_key, axis), (), 0, length) for axis, length in enumerate(array.shape)]
    widest = array.shape.index(max(array.shape))
    beside = index_at[:widest] + [(index_at[widest] + 1) % array.shape[widest]] + index_at[widest + 1:]
    return array.at[tuple(index_at)].set(smallest).at[tuple(beside)].set(largest)


def shard_levels(stream_key, shape, pieces, smallest, largest):
    def one(axis_at, blocks):
        heights = jax.random.uniform(jax.random.fold_in(jax.random.fold_in(stream_key, 6), axis_at), (blocks,), jnp.float32, smallest / len(pieces), largest / len(pieces))
        return jnp.repeat(jnp.exp(heights), shape[axis_at] // blocks).reshape((-1,) + (1,) * (len(shape) - axis_at - 1))

    loudness = one(*pieces[0])
    for cut in pieces[1:]:
        loudness = loudness * one(*cut)
    return loudness


def noise(rng, dims, spread, reach, pieces=(), kind=jnp.bfloat16):
    result = jax.random.normal(rng, dims, jnp.float32) * spread
    if len(pieces) > 0:
        result = shard_levels(rng, dims, pieces, -0.22, 0.18) * result
    return jnp.clip(result, min=-reach, max=reach).astype(kind)


def setup_inputs(seed: int = 0) -> dict:
    key_list = jax.random.split(jax.random.key(seed), 12)
    return {
        "tokens": noise(key_list[0], (PROMPTS, SEQ, D), 1.0, 6.0, ((0, 16), (1, 2))),
        "attn_in": noise(key_list[1], (PROMPTS, SEQ, D), 1.0, 6.0, ((0, 16), (1, 2))),
        "lengths": place_ends(jax.random.randint(key_list[2], (PROMPTS,), SEQ // 4, SEQ + 1), jax.random.fold_in(key_list[2], 1), SEQ // 4, SEQ).astype(jnp.int32),
        "norm_gain": jnp.clip(1.0 + 0.1 * jax.random.normal(key_list[3], (D,), jnp.float32), 0.5, 1.5),
        "attn_gain": jnp.clip(1.0 + 0.1 * jax.random.normal(key_list[4], (D,), jnp.float32), 0.5, 1.5),
        "w_x": noise(key_list[5], (D, D), D ** -0.5, 0.125, ((0, 32),)),
        "conv_w": noise(key_list[6], (4, D), 0.5, 3.0, (), jnp.float32),
        "w_a": noise(key_list[7], (H, HD, HD), HD ** -0.5, 0.375),
        "w_i": noise(key_list[8], (H, HD, HD), HD ** -0.5, 0.375),
        "lru_decay": draw_lru_decay(jax.random.fold_in(key_list[11], 71), 0),
        "w_kv": noise(key_list[10], (D, 2 * HD), D ** -0.5, 0.125),
    }


def rms_norm(values, gain_vec):
    widened = values.astype(jnp.float32)
    inverse = lax.rsqrt(lax.optimization_barrier(jnp.mean(widened * widened, axis=-1, keepdims=True)) + 1e-06)
    return (widened * inverse * gain_vec).astype(jnp.bfloat16)

def rotate_keys(key_rows, positions):
    quarter = key_rows.shape[-1] // 4
    spacing = jnp.exp(-jnp.log(10000.0) * jnp.arange(quarter, dtype=jnp.float32) / quarter)
    angles = positions.astype(jnp.float32)[:, None] * spacing[None, :]
    cosine_rows = jnp.cos(angles)
    sine_rows = jnp.sin(angles)
    first_part = key_rows[:, :quarter]
    second_part = key_rows[:, quarter:2 * quarter]
    return jnp.concatenate([first_part * cosine_rows - second_part * sine_rows, second_part * cosine_rows + first_part * sine_rows, key_rows[:, 2 * quarter:]], axis=1)

def one_prompt(norm_gain, attn_gain, w_x, conv_w, w_a, w_i, lru_decay, w_kv, tokens, attn_in, length):
    seq_len = tokens.shape[0]
    normed = rms_norm(tokens, norm_gain)
    x_proj = jnp.dot(normed, w_x, preferred_element_type=jnp.float32).astype(jnp.bfloat16)
    padded = jnp.concatenate([jnp.zeros((3, D), jnp.bfloat16), x_proj], axis=0)
    conv_sum = conv_w[0] * padded[0:seq_len].astype(jnp.float32)
    for offset in range(1, 4):
        conv_sum = conv_sum + conv_w[offset] * padded[offset:offset + seq_len].astype(jnp.float32)
    x_conv = conv_sum.astype(jnp.bfloat16)
    head_rows = x_conv.astype(jnp.float32).reshape(seq_len, H, HD)
    gate_a = jnp.einsum('lhk,hkj->lhj', head_rows, w_a.astype(jnp.float32)).reshape(seq_len, D)
    gate_i = jnp.einsum('lhk,hkj->lhj', head_rows, w_i.astype(jnp.float32)).reshape(seq_len, D)
    positions = jnp.arange(seq_len, dtype=jnp.int32)
    valid_row = (positions < length).astype(jnp.float32)[:, None]
    log_rate = -8.0 * jax.nn.softplus(-lru_decay) * jax.nn.sigmoid(gate_a)
    keep_rate = jnp.exp(log_rate * valid_row)
    push_term = jnp.sqrt(-jnp.expm1(2.0 * log_rate)) * jax.nn.sigmoid(gate_i) * x_conv.astype(jnp.float32) * valid_row

    def advance(carried, step_pair):
        return (step_pair[0] * carried + step_pair[1], None)
    lru_state = lax.scan(advance, jnp.zeros((D,), jnp.float32), (keep_rate, push_term))[0]
    conv_state = lax.dynamic_slice_in_dim(padded, length.astype(jnp.int32), 3, 0)
    attn_normed = rms_norm(attn_in, attn_gain)
    kv_full = jnp.dot(attn_normed, w_kv, preferred_element_type=jnp.float32)
    kv_rows = jnp.concatenate([rotate_keys(kv_full[:, :HD], positions), kv_full[:, HD:]], axis=1).astype(jnp.bfloat16)
    in_window = ((positions >= length - W) & (positions < length)).astype(jnp.float32)[:, None]
    masked = kv_rows.astype(jnp.float32) * in_window
    lap_count = -(-seq_len // W)
    masked = jnp.concatenate([masked, jnp.zeros((lap_count * W - seq_len, 2 * HD), jnp.float32)], axis=0)
    kv_cache = lax.optimization_barrier(jnp.sum(masked.reshape(lap_count, W, 2 * HD), axis=0)).astype(jnp.bfloat16)
    return (lru_state, conv_state, kv_cache)

def reference(tokens, attn_in, lengths, norm_gain, attn_gain, w_x, conv_w, w_a, w_i, lru_decay, w_kv):

    def per_prompt(inputs):
        return one_prompt(norm_gain, attn_gain, w_x, conv_w, w_a, w_i, lru_decay, w_kv, inputs[0], inputs[1], inputs[2])
    lru_state, conv_state, kv_cache = lax.map(per_prompt, (tokens, attn_in, lengths))
    return (lru_state, conv_state, kv_cache)
```

```python
import functools

import jax
import jax.numpy as jnp
from jax import lax
from jax.experimental import pallas as pl
from jax.experimental.pallas import tpu as pltpu
from jax.sharding import PartitionSpec as P

H = 10
HD = 256
W = 2048
LANES_OF_TIME = 8
TAPS = 4
HALO = 16
STEP_ROWS = 32


def passed_along(block, axis, distance):
    devices = range(lax.axis_size(axis))
    route = [(i - distance, i) for i in devices if i - distance in devices]
    return lax.ppermute(block, axis, route)


def rms_norm(values, gain_vec):
    widened = values.astype(jnp.float32)
    inverse = lax.rsqrt(jnp.mean(widened * widened, axis=-1, keepdims=True) + 1e-06)
    return (widened * inverse * gain_vec).astype(jnp.bfloat16)


def rotate_keys(key_rows, positions):
    quarter = key_rows.shape[-1] // 4
    spacing = jnp.exp(-jnp.log(10000.0) * jnp.arange(quarter, dtype=jnp.float32) / quarter)
    angles = positions.astype(jnp.float32)[:, None] * spacing[None, :]
    cosine_rows = jnp.cos(angles)
    sine_rows = jnp.sin(angles)
    first_part = key_rows[:, :quarter]
    second_part = key_rows[:, quarter : 2 * quarter]
    return jnp.concatenate(
        [
            first_part * cosine_rows - second_part * sine_rows,
            second_part * cosine_rows + first_part * sine_rows,
            key_rows[:, 2 * quarter :],
        ],
        axis=1,
    )


def ordered_rows(tokens_ref, halo_ref, gain_ref, normed_ref):
    local_len = tokens_ref.shape[0]
    steps = local_len // LANES_OF_TIME
    row = lax.broadcasted_iota(jnp.int32, (normed_ref.shape[0], local_len + HALO), 0)
    col = lax.broadcasted_iota(jnp.int32, (normed_ref.shape[0], local_len + HALO), 1)
    at = lax.rem(row, LANES_OF_TIME) * steps + lax.div(row, LANES_OF_TIME) - (TAPS - 1)
    pick = (jnp.where(at < 0, at + local_len + HALO, at) == col).astype(jnp.bfloat16)
    rows = jnp.concatenate(
        [rms_norm(tokens_ref[...], gain_ref[...]), rms_norm(halo_ref[...], gain_ref[...])], axis=0
    )
    normed_ref[...] = jnp.dot(pick, rows, preferred_element_type=jnp.float32).astype(jnp.bfloat16)


def one_head(
    normed_ref, w_block, conv_w, w_a, w_i, rate, length, start, out_ref, xp_ref, xc_ref, ga_ref, gi_ref
):
    rows_ext = normed_ref.shape[0]
    local_len = xc_ref.shape[0]
    steps = local_len // LANES_OF_TIME
    projected = jnp.dot(normed_ref[...], w_block, preferred_element_type=jnp.float32).astype(
        jnp.bfloat16
    )
    xp_ref[...] = projected.astype(jnp.float32)
    row = lax.broadcasted_iota(jnp.int32, (HALO, rows_ext), 1)
    wanted = length - (TAPS - 1) + lax.broadcasted_iota(jnp.int32, (HALO, rows_ext), 0) - 2
    step = lax.div(row, LANES_OF_TIME) - (TAPS - 1)
    at = start + lax.rem(row, LANES_OF_TIME) * steps + step
    real = (step >= 0) & (step < steps) & (wanted < length) & (wanted >= length - (TAPS - 1))
    picker = (real & (at == wanted)).astype(jnp.bfloat16)
    picked = jnp.dot(picker, projected, preferred_element_type=jnp.float32)
    conv_sum = conv_w[0:1] * xp_ref[0:local_len]
    for offset in range(1, TAPS):
        shift = offset * LANES_OF_TIME
        conv_sum = conv_sum + conv_w[offset : offset + 1] * xp_ref[shift : shift + local_len]
    x_conv = conv_sum.astype(jnp.bfloat16)
    xc_ref[...] = x_conv.astype(jnp.float32)
    ga_ref[...] = jnp.dot(x_conv, w_a, preferred_element_type=jnp.float32)
    gi_ref[...] = jnp.dot(x_conv, w_i, preferred_element_type=jnp.float32)
    inner = lax.broadcasted_iota(jnp.int32, (STEP_ROWS, HD), 0)
    first_at = start + lax.rem(inner, LANES_OF_TIME) * steps + lax.div(inner, LANES_OF_TIME)

    def block(i, carry):
        state, rate_sum = carry
        rows = pl.ds(pl.multiple_of(i * STEP_ROWS, STEP_ROWS), STEP_ROWS)
        valid = first_at + i * (STEP_ROWS // LANES_OF_TIME) < length
        log_rate = rate * jax.nn.sigmoid(ga_ref[rows])
        fall = -2.0 * log_rate
        lost = 1.0 - fall * (1.0 / 6.0)
        for order in (5.0, 4.0, 3.0, 2.0):
            lost = 1.0 - fall * (1.0 / order) * lost
        lost = fall * lost
        root = lost * lax.rsqrt(jnp.maximum(lost, 1e-37))
        push = jnp.where(valid, root * jax.nn.sigmoid(gi_ref[rows]) * xc_ref[rows], 0.0)
        held = jnp.where(valid, log_rate, 0.0)
        keep = jnp.exp(held)
        for k in range(STEP_ROWS // LANES_OF_TIME):
            tile = slice(k * LANES_OF_TIME, (k + 1) * LANES_OF_TIME)
            state = keep[tile] * state + push[tile]
            rate_sum = rate_sum + held[tile]
        return state, rate_sum

    zeros = jnp.zeros((LANES_OF_TIME, HD), jnp.float32)
    state, rate_sum = lax.fori_loop(0, local_len // STEP_ROWS, block, (zeros, zeros))
    keep_all = jnp.exp(rate_sum)
    total = state[0:1]
    for s in range(1, LANES_OF_TIME):
        total = keep_all[s : s + 1] * total + state[s : s + 1]
    keep_total = jnp.exp(jnp.sum(rate_sum, axis=0, keepdims=True))
    place = lax.broadcasted_iota(jnp.int32, (LANES_OF_TIME, HD), 0)
    out_ref[...] = jnp.where(
        place == 0, keep_total, jnp.where(place == 1, total, picked[0:LANES_OF_TIME])
    )


def recurrent_kernel(
    length_ref,
    tokens_ref,
    halo_ref,
    gain_ref,
    w_ref,
    conv_ref,
    wa_ref,
    wi_ref,
    rate_ref,
    out_ref,
    normed_ref,
    *work
):
    @pl.when(pl.program_id(0) == 0)
    def _():
        ordered_rows(tokens_ref, halo_ref, gain_ref, normed_ref)

    start = lax.axis_index("seq") * tokens_ref.shape[0]
    one_head(
        normed_ref,
        w_ref[...],
        conv_ref[...],
        wa_ref[0],
        wi_ref[0],
        rate_ref[...],
        length_ref[0],
        start,
        out_ref,
        *work
    )


def recurrent(tokens, halo, lengths, norm_gain, w_full, conv_w, w_a, w_i, rate):
    local_len, width = tokens.shape
    rows_ext = -(-(local_len + (TAPS - 1) * LANES_OF_TIME) // HALO) * HALO
    whole = lambda *shape: pl.BlockSpec(shape, lambda h: (0,) * len(shape))
    return pl.pallas_call(
        recurrent_kernel,
        grid=(width // HD,),
        in_specs=[
            pl.BlockSpec(memory_space=pltpu.SMEM),
            whole(local_len, width),
            whole(HALO, width),
            whole(1, width),
            pl.BlockSpec((width, HD), lambda h: (0, h)),
            pl.BlockSpec((TAPS, HD), lambda h: (0, h)),
            pl.BlockSpec((1, HD, HD), lambda h: (h, 0, 0)),
            pl.BlockSpec((1, HD, HD), lambda h: (h, 0, 0)),
            pl.BlockSpec((1, HD), lambda h: (0, h)),
        ],
        out_specs=pl.BlockSpec((LANES_OF_TIME, HD), lambda h: (0, h)),
        out_shape=jax.ShapeDtypeStruct((LANES_OF_TIME, width), jnp.float32),
        scratch_shapes=[
            pltpu.VMEM((rows_ext, width), jnp.bfloat16),
            pltpu.VMEM((rows_ext, HD), jnp.float32),
            pltpu.VMEM((local_len, HD), jnp.float32),
            pltpu.VMEM((local_len, HD), jnp.float32),
            pltpu.VMEM((local_len, HD), jnp.float32),
        ],
        compiler_params=pltpu.CompilerParams(vmem_limit_bytes=48 * 1024 * 1024),
    )(lengths, tokens, halo, norm_gain[None], w_full, conv_w, w_a, w_i, rate[None])


def on_device(
    tokens, attn_in, lengths, norm_gain, attn_gain, w_x, conv_w, w_a, w_i, lru_decay, w_kv
):
    local_len = tokens.shape[1]
    feature_dim = tokens.shape[2]
    seq_parts = lax.axis_size("seq")
    seq_place = lax.axis_index("seq")
    length = lengths[0]
    halo = passed_along(tokens[0, local_len - HALO :], "seq", 1)
    w_full = lax.all_gather(w_x, ("batch", "seq"), axis=0, tiled=True)
    positions = seq_place * local_len + jnp.arange(local_len, dtype=jnp.int32)
    attn_normed = rms_norm(attn_in[0], attn_gain)
    kv_full = jnp.dot(attn_normed, w_kv, preferred_element_type=jnp.float32)
    kv_rows = jnp.concatenate(
        [rotate_keys(kv_full[:, :HD], positions), kv_full[:, HD:]], axis=1
    ).astype(jnp.bfloat16)
    in_window = ((positions >= length - W) & (positions < length))[:, None]
    masked = jnp.where(in_window, kv_rows, jnp.zeros_like(kv_rows))
    by_column = lax.all_to_all(masked, "seq", split_axis=1, concat_axis=0, tiled=True)
    laps = -(-seq_parts * local_len // W)
    by_column = jnp.pad(by_column, ((0, laps * W - seq_parts * local_len), (0, 0)))
    kv_cache = by_column[:W]
    for lap in range(1, laps):
        kv_cache = kv_cache + by_column[lap * W : (lap + 1) * W]
    rate = -8.0 * jax.nn.softplus(-lru_decay)
    summary = recurrent(tokens[0], halo, lengths, norm_gain, w_full, conv_w, w_a, w_i, rate)
    owned = lax.all_to_all(
        summary.reshape(1, LANES_OF_TIME, feature_dim), "seq", split_axis=2, concat_axis=0, tiled=True
    )
    state = owned[0, 1]
    for part in range(1, seq_parts):
        state = owned[part, 0] * state + owned[part, 1]
    conv_state = jnp.sum(owned[:, 2:5], axis=0).astype(jnp.bfloat16)
    return (state[None], conv_state[None], kv_cache[None])


def solution(mesh):
    in_specs = (
        P("batch", "seq", None),
        P("batch", "seq", None),
        P("batch"),
        P(),
        P(),
        P(("batch", "seq"), None),
        P(),
        P(),
        P(),
        P(),
        P(),
    )
    out_specs = (P("batch", "seq"), P("batch", None, "seq"), P("batch", None, "seq"))
    return jax.shard_map(
        on_device, mesh=mesh, in_specs=in_specs, out_specs=out_specs, check_vma=False
    )
```

```python
import functools

import jax
import jax.numpy as jnp
from jax import lax
from jax.experimental import pallas as pl
from jax.experimental.pallas import tpu as pltpu
from jax.sharding import PartitionSpec as P

H = 10
HD = 256
W = 2048
LANES_OF_TIME = 8
TAPS = 4
HALO = 16
STEP_ROWS = 32


def passed_along(block, axis, distance):
    devices = range(lax.axis_size(axis))
    route = [(i - distance, i) for i in devices if i - distance in devices]
    return lax.ppermute(block, axis, route)


def rms_norm(values, gain_vec):
    widened = values.astype(jnp.float32)
    inverse = lax.rsqrt(jnp.mean(widened * widened, axis=-1, keepdims=True) + 1e-06)
    return (widened * inverse * gain_vec).astype(jnp.bfloat16)


def rotate_keys(key_rows, positions):
    quarter = key_rows.shape[-1] // 4
    spacing = jnp.exp(-jnp.log(10000.0) * jnp.arange(quarter, dtype=jnp.float32) / quarter)
    angles = positions.astype(jnp.float32)[:, None] * spacing[None, :]
    cosine_rows = jnp.cos(angles)
    sine_rows = jnp.sin(angles)
    first_part = key_rows[:, :quarter]
    second_part = key_rows[:, quarter : 2 * quarter]
    return jnp.concatenate(
        [
            first_part * cosine_rows - second_part * sine_rows,
            second_part * cosine_rows + first_part * sine_rows,
            key_rows[:, 2 * quarter :],
        ],
        axis=1,
    )


def ordered_rows(tokens_ref, halo_ref, gain_ref, normed_ref):
    local_len = tokens_ref.shape[0]
    steps = local_len // LANES_OF_TIME
    row = lax.broadcasted_iota(jnp.int32, (normed_ref.shape[0], local_len + HALO), 0)
    col = lax.broadcasted_iota(jnp.int32, (normed_ref.shape[0], local_len + HALO), 1)
    at = lax.rem(row, LANES_OF_TIME) * steps + lax.div(row, LANES_OF_TIME) - (TAPS - 1)
    pick = (jnp.where(at < 0, at + local_len + HALO, at) == col).astype(jnp.bfloat16)
    rows = jnp.concatenate(
        [rms_norm(tokens_ref[...], gain_ref[...]), rms_norm(halo_ref[...], gain_ref[...])], axis=0
    )
    normed_ref[...] = jnp.dot(pick, rows, preferred_element_type=jnp.float32).astype(jnp.bfloat16)


def one_head(
    normed_ref, w_block, conv_w, w_a, w_i, rate, length, start, out_ref, xp_ref, xc_ref, ga_ref, gi_ref
):
    rows_ext = normed_ref.shape[0]
    local_len = xc_ref.shape[0]
    steps = local_len // LANES_OF_TIME
    projected = jnp.dot(normed_ref[...], w_block, preferred_element_type=jnp.float32).astype(
        jnp.bfloat16
    )
    xp_ref[...] = projected.astype(jnp.float32)
    row = lax.broadcasted_iota(jnp.int32, (HALO, rows_ext), 1)
    wanted = length - (TAPS - 1) + lax.broadcasted_iota(jnp.int32, (HALO, rows_ext), 0) - 2
    step = lax.div(row, LANES_OF_TIME) - (TAPS - 1)
    at = start + lax.rem(row, LANES_OF_TIME) * steps + step
    real = (step >= 0) & (step < steps) & (wanted < length) & (wanted >= length - (TAPS - 1))
    picker = (real & (at == wanted)).astype(jnp.bfloat16)
    picked = jnp.dot(picker, projected, preferred_element_type=jnp.float32)
    conv_sum = conv_w[0:1] * xp_ref[0:local_len]
    for offset in range(1, TAPS):
        shift = offset * LANES_OF_TIME
        conv_sum = conv_sum + conv_w[offset : offset + 1] * xp_ref[shift : shift + local_len]
    x_conv = conv_sum.astype(jnp.bfloat16)
    xc_ref[...] = x_conv.astype(jnp.float32)
    ga_ref[...] = jnp.dot(x_conv, w_a, preferred_element_type=jnp.float32)
    gi_ref[...] = jnp.dot(x_conv, w_i, preferred_element_type=jnp.float32)
    inner = lax.broadcasted_iota(jnp.int32, (STEP_ROWS, HD), 0)
    first_at = start + lax.rem(inner, LANES_OF_TIME) * steps + lax.div(inner, LANES_OF_TIME)

    def block(i, carry):
        state, rate_sum = carry
        rows = pl.ds(pl.multiple_of(i * STEP_ROWS, STEP_ROWS), STEP_ROWS)
        valid = first_at + i * (STEP_ROWS // LANES_OF_TIME) < length
        log_rate = rate * jax.nn.sigmoid(ga_ref[rows])
        fall = -2.0 * log_rate
        lost = 1.0 - fall * (1.0 / 6.0)
        for order in (5.0, 4.0, 3.0, 2.0):
            lost = 1.0 - fall * (1.0 / order) * lost
        lost = fall * lost
        root = lost * lax.rsqrt(jnp.maximum(lost, 1e-37))
        push = jnp.where(valid, root * jax.nn.sigmoid(gi_ref[rows]) * xc_ref[rows], 0.0)
        held = jnp.where(valid, log_rate, 0.0)
        keep = jnp.exp(held)
        for k in range(STEP_ROWS // LANES_OF_TIME):
            tile = slice(k * LANES_OF_TIME, (k + 1) * LANES_OF_TIME)
            state = keep[tile] * state + push[tile]
            rate_sum = rate_sum + held[tile]
        return state, rate_sum

    zeros = jnp.zeros((LANES_OF_TIME, HD), jnp.float32)
    state, rate_sum = lax.fori_loop(0, local_len // STEP_ROWS, block, (zeros, zeros))
    keep_all = jnp.exp(rate_sum)
    total = state[0:1]
    for s in range(1, LANES_OF_TIME):
        total = keep_all[s : s + 1] * total + state[s : s + 1]
    keep_total = jnp.exp(jnp.sum(rate_sum, axis=0, keepdims=True))
    place = lax.broadcasted_iota(jnp.int32, (LANES_OF_TIME, HD), 0)
    out_ref[...] = jnp.where(
        place == 0, keep_total, jnp.where(place == 1, total, picked[0:LANES_OF_TIME])
    )


def recurrent_kernel(
    length_ref,
    tokens_ref,
    halo_ref,
    gain_ref,
    w_ref,
    conv_ref,
    wa_ref,
    wi_ref,
    rate_ref,
    out_ref,
    normed_ref,
    *work
):
    @pl.when(pl.program_id(0) == 0)
    def _():
        ordered_rows(tokens_ref, halo_ref, gain_ref, normed_ref)

    start = lax.axis_index("seq") * tokens_ref.shape[0]
    one_head(
        normed_ref,
        w_ref[...],
        conv_ref[...],
        wa_ref[0],
        wi_ref[0],
        rate_ref[...],
        length_ref[0],
        start,
        out_ref,
        *work
    )


def recurrent(first, tokens, halo, lengths, norm_gain, w_part, conv_w, w_a, w_i, rate):
    local_len, width = tokens.shape
    part_width = w_part.shape[1]
    rows_ext = -(-(local_len + (TAPS - 1) * LANES_OF_TIME) // HALO) * HALO
    whole = lambda *shape: pl.BlockSpec(shape, lambda h: (0,) * len(shape))
    return pl.pallas_call(
        recurrent_kernel,
        grid=(part_width // HD,),
        in_specs=[
            pl.BlockSpec(memory_space=pltpu.SMEM),
            whole(local_len, width),
            whole(HALO, width),
            whole(1, width),
            pl.BlockSpec((width, HD), lambda h: (0, h)),
            pl.BlockSpec((TAPS, HD), lambda h: (0, h + first)),
            pl.BlockSpec((1, HD, HD), lambda h: (h + first, 0, 0)),
            pl.BlockSpec((1, HD, HD), lambda h: (h + first, 0, 0)),
            pl.BlockSpec((1, HD), lambda h: (0, h + first)),
        ],
        out_specs=pl.BlockSpec((LANES_OF_TIME, HD), lambda h: (0, h)),
        out_shape=jax.ShapeDtypeStruct((LANES_OF_TIME, part_width), jnp.float32),
        scratch_shapes=[
            pltpu.VMEM((rows_ext, width), jnp.bfloat16),
            pltpu.VMEM((rows_ext, HD), jnp.float32),
            pltpu.VMEM((local_len, HD), jnp.float32),
            pltpu.VMEM((local_len, HD), jnp.float32),
            pltpu.VMEM((local_len, HD), jnp.float32),
        ],
        compiler_params=pltpu.CompilerParams(vmem_limit_bytes=60 * 1024 * 1024),
        cost_estimate=pl.CostEstimate(
            flops=2 * local_len * part_width * (width + 2 * HD),
            bytes_accessed=2 * width * (local_len + part_width),
            transcendentals=6 * local_len * part_width,
        ),
    )(lengths, tokens, halo, norm_gain[None], w_part, conv_w, w_a, w_i, rate[None])


def on_device(
    tokens, attn_in, lengths, norm_gain, attn_gain, w_x, conv_w, w_a, w_i, lru_decay, w_kv
):
    local_len = tokens.shape[1]
    feature_dim = tokens.shape[2]
    seq_parts = lax.axis_size("seq")
    seq_place = lax.axis_index("seq")
    length = lengths[0]
    halo = passed_along(tokens[0, local_len - HALO :], "seq", 1)
    heads = feature_dim // HD
    early = (4 * heads) // 5
    positions = seq_place * local_len + jnp.arange(local_len, dtype=jnp.int32)
    attn_normed = rms_norm(attn_in[0], attn_gain)
    kv_full = jnp.dot(attn_normed, w_kv, preferred_element_type=jnp.float32)
    kv_rows = jnp.concatenate(
        [rotate_keys(kv_full[:, :HD], positions), kv_full[:, HD:]], axis=1
    ).astype(jnp.bfloat16)
    in_window = ((positions >= length - W) & (positions < length))[:, None]
    masked = jnp.where(in_window, kv_rows, jnp.zeros_like(kv_rows))
    by_column = lax.all_to_all(masked, "seq", split_axis=1, concat_axis=0, tiled=True)
    laps = -(-seq_parts * local_len // W)
    by_column = jnp.pad(by_column, ((0, laps * W - seq_parts * local_len), (0, 0)))
    kv_cache = by_column[:W]
    for lap in range(1, laps):
        kv_cache = kv_cache + by_column[lap * W : (lap + 1) * W]
    w_early = lax.all_gather(w_x[:, : early * HD], ("batch", "seq"), axis=0, tiled=True)
    w_early, w_local, kv_cache, halo = lax.optimization_barrier((w_early, w_x, kv_cache, halo))
    w_late = lax.all_gather(w_local[:, early * HD :], ("batch", "seq"), axis=0, tiled=True)
    w_parts = ((0, w_early), (early, w_late))
    rate = -8.0 * jax.nn.softplus(-lru_decay)
    summary = jnp.concatenate(
        [
            recurrent(first, tokens[0], halo, lengths, norm_gain, w_part, conv_w, w_a, w_i, rate)
            for first, w_part in w_parts
        ],
        axis=1,
    )
    owned_width = feature_dim // seq_parts
    gathered = lax.all_gather(summary, "seq", axis=0, tiled=True)
    owned = lax.dynamic_slice_in_dim(gathered, seq_place * owned_width, owned_width, 1)
    state = owned[1:2]
    picked = owned[2:5]
    for part in range(1, seq_parts):
        at = part * LANES_OF_TIME
        state = owned[at : at + 1] * state + owned[at + 1 : at + 2]
        picked = picked + owned[at + 2 : at + 5]
    conv_state = picked.astype(jnp.bfloat16)
    return (state, conv_state[None], kv_cache[None])


def solution(mesh):
    in_specs = (
        P("batch", "seq", None),
        P("batch", "seq", None),
        P("batch"),
        P(),
        P(),
        P(("batch", "seq"), None),
        P(),
        P(),
        P(),
        P(),
        P(),
    )
    out_specs = (P("batch", "seq"), P("batch", None, "seq"), P("batch", None, "seq"))
    return jax.shard_map(
        on_device, mesh=mesh, in_specs=in_specs, out_specs=out_specs, check_vma=False
    )
```
